32 devices in a mesh: seq: 16 (over z, y, core), head: 2 (over x).
Axes of the slice: x: 2, y: 2, z: 4, core: 2. Of those that a mesh axis runs over, the one named last changes fastest.
Arguments:
- sequence: bfloat16 [8192, 2048], P('seq'), may hold values from -6 to 6
- input_weight: bfloat16 [2048, 4096], P(None, 'head'), may hold values from -0.125 to 0.125
- gate_weight: bfloat16 [2048, 4096], P(None, 'head'), may hold values from -0.125 to 0.125
- state_weight: bfloat16 [2048, 256], replicated, may hold values from -0.015625 to 0.015625
- step_weight: bfloat16 [2048, 64], P(None, 'head'), may hold values from -0.125 to 0.125
- step_bias: float32 [64], P('head'), may hold values from -2 to 0
- decay_rate: float32 [64], P('head'), may hold values from 6.1035156e-05 to 0.1
- skip_gain: float32 [64], P('head'), may hold values from 0.5 to 1.5
- output_weight: bfloat16 [4096, 2048], P('head'), may hold values from -0.09375 to 0.09375
Outputs:
- encoded: bfloat16 [8192, 2048], P('seq', 'head')
The draws below stay inside these ranges and needn't reach their ends.
All inputs are finite; a program needn't handle non-finite values.
Results may differ from the reference program's by a relative error of at most 0.014.
Values sent between devices are 32-bit elements; how exact they have to be, the bound alone decides.
A program may use at most 128 MiB of HBM per device.

```python
import math
import jax
import jax.numpy as jnp
from jax import lax

D = 2048
HEADS = 64
HEADDIM = 64
STATE = 128
SEQ_DEV = 512
LENGTH = 8192


def steps_of(key, dims, cuts, least, high):
    loudness = 1.0
    for dim, parts in cuts:
        heights = jax.random.uniform(jax.random.fold_in(jax.random.fold_in(key, 6), dim), (parts,), jnp.float32, least / len(cuts), high / len(cuts))
        loudness = loudness * jnp.repeat(jnp.exp(heights), dims[dim] // parts).reshape((-1,) + (1,) * (len(dims) - 1 - dim))
    return loudness


def bell_draw(stream_key, extent, scale, most, shards=(), kind=jnp.bfloat16):
    gain = steps_of(stream_key, extent, shards, -0.22, 0.18) if shards else 1.0
    array = jax.random.normal(stream_key, extent, jnp.float32) * scale * gain
    return jnp.minimum(jnp.maximum(array, -most), most).astype(kind)


def setup_inputs(seed: int = 0) -> dict:
    splits = jax.random.split(jax.random.key(seed), 10)
    return {
        "sequence": bell_draw(splits[0], (LENGTH, D), 1.0, 6.0, ((0, 16),)),
        "input_weight": bell_draw(splits[1], (D, HEADS * HEADDIM), D ** -0.5, 0.125, ((1, 2),)),
        "gate_weight": bell_draw(splits[2], (D, HEADS * HEADDIM), D ** -0.5, 0.125, ((1, 2),)),
        "state_weight": bell_draw(splits[3], (D, 2 * STATE), (D * 64) ** -0.5, 0.015625),
        "step_weight": bell_draw(splits[4], (D, HEADS), D ** -0.5, 0.125, ((1, 2),)),
        "step_bias": jnp.clip(-2.0 + 2.0 * jax.random.uniform(splits[5], (HEADS,), jnp.float32) ** steps_of(splits[5], (HEADS,), ((0, 2),), -0.2, 0.2), -2.0, 0.0),
        "decay_rate": jnp.clip(jnp.exp(math.log(0.1) - 7.4014754 * jax.random.uniform(splits[6], (HEADS,), jnp.float32) ** steps_of(splits[6], (HEADS,), ((0, 2),), -0.2, 0.2)), 6.103515625e-05, 0.1),
        "skip_gain": jnp.clip(0.5 + 1.0 * jax.random.uniform(splits[7], (HEADS,), jnp.float32) ** steps_of(splits[7], (HEADS,), ((0, 2),), -0.2, 0.2), 0.5, 1.5),
        "output_weight": bell_draw(splits[8], (HEADS * HEADDIM, D), (HEADS * HEADDIM) ** -0.5, 0.09375, ((0, 2),)),
    }


def project(sequence, input_weight, gate_weight, state_weight, step_weight, step_bias):
    inputs = jnp.dot(sequence, input_weight, preferred_element_type=jnp.float32).astype(jnp.bfloat16)
    gates = jnp.dot(sequence, gate_weight, preferred_element_type=jnp.float32).astype(jnp.bfloat16)
    state_proj = jnp.dot(sequence, state_weight, preferred_element_type=jnp.float32).astype(jnp.bfloat16)
    raw_steps = jnp.dot(sequence, step_weight, preferred_element_type=jnp.float32) + step_bias[None, :]
    step_sizes = jax.nn.softplus(raw_steps).astype(jnp.bfloat16)
    return inputs, gates, state_proj, step_sizes


def group_parts(inputs, state_proj, step_sizes, decay_rate):
    row_count, head_count = step_sizes.shape
    state_size = state_proj.shape[1] // 2
    per_head = inputs.reshape(row_count, head_count, -1)
    writer = state_proj[:, :state_size]
    reader = state_proj[:, state_size:]
    step_float = step_sizes.astype(jnp.float32)
    log_decay = jnp.cumsum(-decay_rate[None, :] * step_float, axis=0)
    by_head = log_decay.T
    affinity = jnp.dot(reader, writer.T, preferred_element_type=jnp.float32)
    causal = lax.broadcasted_iota(jnp.int32, (row_count, row_count), 0) >= lax.broadcasted_iota(jnp.int32, (row_count, row_count), 1)
    spread = jnp.where(causal[None], by_head[:, :, None] - by_head[:, None, :], jnp.float32(0.0))
    decays = jnp.where(causal[None], jnp.exp(spread), jnp.float32(0.0))
    mixing = (affinity[None] * decays * step_float.T[:, None, :]).astype(jnp.bfloat16)
    inside = jnp.einsum("hts,shp->thp", mixing.astype(jnp.float32), per_head.astype(jnp.float32))
    to_end = jnp.exp(log_decay[-1][None, :] - log_decay) * step_float
    weighted = (per_head.astype(jnp.float32) * to_end[:, :, None]).astype(jnp.bfloat16)
    local_state = jnp.einsum("shp,sn->hpn", weighted.astype(jnp.float32), writer.astype(jnp.float32))
    totals = jnp.exp(log_decay[-1])
    return inside, log_decay, totals, local_state


def finish(inside, log_decay, carry_in, state_proj, inputs, gates, skip_gain):
    row_count, head_count = log_decay.shape
    state_size = state_proj.shape[1] // 2
    reader = state_proj[:, state_size:].astype(jnp.float32)
    per_head = inputs.reshape(row_count, head_count, -1).astype(jnp.float32)
    carried = jnp.einsum("tn,hpn->thp", reader, carry_in, precision=lax.Precision.HIGHEST)
    result = inside + jnp.exp(log_decay)[:, :, None] * carried + skip_gain[None, :, None] * per_head
    result = result.reshape(row_count, -1)
    return (result * jax.nn.silu(gates.astype(jnp.float32))).astype(jnp.bfloat16)


def branch(sequence, input_weight, gate_weight, state_weight, step_weight, step_bias, decay_rate, skip_gain):
    inputs, gates, state_proj, step_sizes = project(sequence, input_weight, gate_weight, state_weight, step_weight, step_bias)
    group_count = sequence.shape[0] // SEQ_DEV

    def advance(carry_in, pieces):
        part_in, part_gate, part_state, part_step = pieces
        inside, log_decay, totals, local_state = group_parts(part_in, part_state, part_step, decay_rate)
        out_rows = finish(inside, log_decay, carry_in, part_state, part_in, part_gate, skip_gain)
        return totals[:, None, None] * carry_in + local_state, out_rows

    pieces = (inputs.reshape(group_count, SEQ_DEV, inputs.shape[1]),
              gates.reshape(group_count, SEQ_DEV, gates.shape[1]),
              state_proj.reshape(group_count, SEQ_DEV, state_proj.shape[1]),
              step_sizes.reshape(group_count, SEQ_DEV, step_sizes.shape[1]))
    start = jnp.zeros((HEADS, HEADDIM, STATE), jnp.float32)
    final_state, rows_out = lax.scan(advance, start, pieces)
    return rows_out.reshape(sequence.shape[0], -1)


def reference(sequence, input_weight, gate_weight, state_weight, step_weight, step_bias, decay_rate, skip_gain, output_weight):
    forward = branch(sequence, input_weight, gate_weight, state_weight, step_weight, step_bias, decay_rate, skip_gain)
    mirrored = sequence[::-1, ::-1]
    backward_mirror = branch(mirrored, input_weight, gate_weight, state_weight, step_weight, step_bias, decay_rate, skip_gain)
    backward = backward_mirror[::-1]
    summed = jnp.dot(forward, output_weight, preferred_element_type=jnp.float32)
    summed = summed + jnp.dot(backward, output_weight[:, ::-1], preferred_element_type=jnp.float32)
    return summed.astype(jnp.bfloat16)
```

```python
import functools

import jax
import jax.numpy as jnp
from jax import lax
from jax.experimental import pallas as pl
from jax.experimental.pallas import tpu as pltpu
from jax.sharding import PartitionSpec as P

F32 = jnp.float32
BF16 = jnp.bfloat16
HEADDIM = 64
CHUNK = 128


def eye_flip(size):
    r = lax.broadcasted_iota(jnp.int32, (size, size), 0)
    c = lax.broadcasted_iota(jnp.int32, (size, size), 1)
    return jnp.where(r + c == size - 1, 1.0, 0.0).astype(BF16)


def flip_kernel(s_ref, o_ref):
    rows, width = s_ref.shape
    block = min(256, width)
    flip = eye_flip(block)
    count = width // block
    o_ref[:rows, :] = s_ref[...]
    for b in range(count):
        src = s_ref[:, (count - 1 - b) * block : (count - b) * block]
        o_ref[rows:, b * block : (b + 1) * block] = jnp.dot(
            src, flip, preferred_element_type=F32
        ).astype(BF16)


def stacked(sequence):
    rows, width = sequence.shape
    return pl.pallas_call(
        flip_kernel,
        out_shape=jax.ShapeDtypeStruct((2 * rows, width), BF16),
    )(sequence)


def pair_wide(cols, first):
    rows = cols.shape[0]
    lane = lax.broadcasted_iota(jnp.int32, (rows, 2 * HEADDIM), 1)
    return jnp.where(lane < HEADDIM, cols[:, first : first + 1], cols[:, first + 1 : first + 2])


def state_kernel(pairs, x_ref, b_ref, w_ref, o_ref):
    writer = b_ref[...]
    factor = w_ref[0]
    parts = []
    for p in range(pairs):
        x = x_ref[:, p * 128 : (p + 1) * 128].astype(F32)
        parts.append((x * pair_wide(factor, 2 * p)).astype(BF16))
    weighted = jnp.concatenate(parts, axis=1)
    o_ref[0] = lax.dot_general(
        writer, weighted, (((0,), (0,)), ((), ())), preferred_element_type=F32
    )


def local_states(inputs, state_proj, factor, rows):
    width = inputs.shape[1]
    state = state_proj.shape[1] // 2
    pairs = min(4, width // 128)
    groups = width // (128 * pairs)
    return pl.pallas_call(
        functools.partial(state_kernel, pairs),
        grid=(2, groups),
        in_specs=[
            pl.BlockSpec((rows, 128 * pairs), lambda d, g: (d, g)),
            pl.BlockSpec((rows, state), lambda d, g: (d, 0)),
            pl.BlockSpec((1, rows, 2 * pairs), lambda d, g: (d * groups + g, 0, 0)),
        ],
        out_specs=pl.BlockSpec((1, state, 128 * pairs), lambda d, g: (d, 0, g)),
        out_shape=jax.ShapeDtypeStruct((2, state, width), F32),
        compiler_params=pltpu.CompilerParams(dimension_semantics=("arbitrary", "arbitrary")),
    )(inputs, state_proj, factor)


def inside_kernel(pairs, state, x_ref, s_ref, ld_ref, ldt_ref, dt_ref, dtt_ref, skip_ref, o_ref, aff):
    branch = pl.program_id(0)
    rows = x_ref.shape[0]
    count = rows // CHUNK
    r = lax.broadcasted_iota(jnp.int32, (CHUNK, CHUNK), 0)
    c = lax.broadcasted_iota(jnp.int32, (CHUNK, CHUNK), 1)

    @pl.when(pl.program_id(1) == 0)
    def _():
        for k in range(count):
            at = slice(k * CHUNK, (k + 1) * CHUNK)
            aff[k] = lax.dot_general(
                s_ref[at, state:], s_ref[at, :state], (((1,), (1,)), ((), ())),
                preferred_element_type=F32,
            )

    lane = lax.broadcasted_iota(jnp.int32, (CHUNK, 128), 1)

    def run(ahead):
        keep = (r >= c) if ahead else (r <= c)
        ld = ld_ref[0]
        ldt = ldt_ref[0]
        dt = dt_ref[0]
        dtt = dtt_ref[0]
        order = range(count) if ahead else range(count - 1, -1, -1)
        carry = jnp.zeros((state, 128 * pairs), F32)
        edge_prev = None
        for step, k in enumerate(order):
            at = slice(k * CHUNK, (k + 1) * CHUNK)
            edge_row = (k + 1) * CHUNK - 1 if ahead else k * CHUNK
            ldk = ld[at, :]
            edge = ld[edge_row : edge_row + 1, :]
            since = jnp.exp(ldk) if step == 0 else jnp.exp(ldk - edge_prev)
            to_end = jnp.exp(edge - ldk) * dt[at, :]
            if step:
                carried = jnp.dot(s_ref[at, state:], carry.astype(BF16), preferred_element_type=F32)
            weighted = []
            for p in range(pairs):
                cols = slice(p * 128, (p + 1) * 128)
                x = x_ref[at, cols]
                xf = x.astype(F32)
                mixes = []
                for h in (2 * p, 2 * p + 1):
                    spread = jnp.where(keep, ldk[:, h : h + 1] - ldt[h : h + 1, at], 0.0)
                    mix = jnp.where(keep, aff[k] * jnp.exp(spread), 0.0) * dtt[h : h + 1, at]
                    mixes.append(mix.astype(BF16))
                zero = jnp.zeros_like(x)
                both = jnp.concatenate(
                    [jnp.where(lane < HEADDIM, x, zero), jnp.where(lane < HEADDIM, zero, x)], axis=0
                )
                out = jnp.dot(jnp.concatenate(mixes, axis=1), both, preferred_element_type=F32)
                out = out + xf * skip_ref[:, cols]
                if step:
                    out = out + carried[:, cols] * pair_wide(since, 2 * p)
                o_ref[at, cols] = out.astype(BF16)
                if step < count - 1:
                    weighted.append((xf * pair_wide(to_end, 2 * p)).astype(BF16))
            if step < count - 1:
                local = lax.dot_general(
                    s_ref[at, :state], jnp.concatenate(weighted, axis=1),
                    (((0,), (0,)), ((), ())), preferred_element_type=F32,
                )
                if step:
                    fade = jnp.exp(edge - edge_prev)
                    wide = jnp.concatenate([pair_wide(fade, 2 * p) for p in range(pairs)], axis=1)
                    carry = carry * wide + local
                else:
                    carry = local
            edge_prev = edge

    @pl.when(branch == 0)
    def _():
        run(True)

    @pl.when(branch == 1)
    def _():
        run(False)


def inside_of(inputs, state_proj, ld, ldt, dt, dtt, skip, rows):
    width = inputs.shape[1]
    state = state_proj.shape[1] // 2
    pairs = min(4, width // 128)
    groups = width // (128 * pairs)
    heads = 2 * pairs
    return pl.pallas_call(
        functools.partial(inside_kernel, pairs, state),
        grid=(2, groups),
        in_specs=[
            pl.BlockSpec((rows, 128 * pairs), lambda d, g: (d, g)),
            pl.BlockSpec((rows, 2 * state), lambda d, g: (d, 0)),
            pl.BlockSpec((1, rows, heads), lambda d, g: (d * groups + g, 0, 0)),
            pl.BlockSpec((1, heads, rows), lambda d, g: (d * groups + g, 0, 0)),
            pl.BlockSpec((1, rows, heads), lambda d, g: (d * groups + g, 0, 0)),
            pl.BlockSpec((1, heads, rows), lambda d, g: (d * groups + g, 0, 0)),
            pl.BlockSpec((1, 128 * pairs), lambda d, g: (0, g)),
        ],
        out_specs=pl.BlockSpec((rows, 128 * pairs), lambda d, g: (d, g)),
        out_shape=jax.ShapeDtypeStruct(inputs.shape, BF16),
        scratch_shapes=[pltpu.VMEM((rows // CHUNK, CHUNK, CHUNK), F32)],
        compiler_params=pltpu.CompilerParams(dimension_semantics=("arbitrary", "arbitrary")),
    )(inputs, state_proj, ld, ldt, dt, dtt, skip)


def gate_kernel(pairs, state, i_ref, g_ref, s_ref, ld_ref, c_ref, o_ref):
    reader = s_ref[:, state:]
    carried = jnp.dot(reader, c_ref[0].astype(BF16), preferred_element_type=F32)
    grown = jnp.exp(ld_ref[0])
    for p in range(pairs):
        cols = slice(p * 128, (p + 1) * 128)
        g = g_ref[:, cols].astype(F32)
        full = i_ref[:, cols].astype(F32) + carried[:, cols] * pair_wide(grown, 2 * p)
        o_ref[:, cols] = (full * (g / (1.0 + jnp.exp(-g)))).astype(BF16)


def gated_of(inside, gates, state_proj, ld, carry, rows):
    width = inside.shape[1]
    state = state_proj.shape[1] // 2
    pairs = min(4, width // 128)
    groups = width // (128 * pairs)
    heads = 2 * pairs
    tile = pl.BlockSpec((rows, 128 * pairs), lambda d, g: (d, g))
    return pl.pallas_call(
        functools.partial(gate_kernel, pairs, state),
        grid=(2, groups),
        in_specs=[
            tile,
            tile,
            pl.BlockSpec((rows, 2 * state), lambda d, g: (d, 0)),
            pl.BlockSpec((1, rows, heads), lambda d, g: (d * groups + g, 0, 0)),
            pl.BlockSpec((1, state, 128 * pairs), lambda d, g: (d, 0, g)),
        ],
        out_specs=tile,
        out_shape=jax.ShapeDtypeStruct(inside.shape, BF16),
        compiler_params=pltpu.CompilerParams(dimension_semantics=("arbitrary", "arbitrary")),
    )(inside, gates, state_proj, ld, carry)


def out_kernel(rows, at_ref, g_ref, w_ref, v_ref, o_ref):
    flipped = jnp.dot(v_ref[...], eye_flip(v_ref.shape[1]), preferred_element_type=F32).astype(BF16)
    acc = jnp.dot(g_ref[:rows, :], w_ref[...], preferred_element_type=F32)
    o_ref[...] = acc + jnp.dot(g_ref[rows:, :], flipped, preferred_element_type=F32)


def out_share(gated, weight, share, shares, rows):
    depth, columns = weight.shape
    wide = columns // shares
    block = min(256, wide)
    per = wide // block
    total = columns // block
    return pl.pallas_call(
        functools.partial(out_kernel, rows),
        grid_spec=pltpu.PrefetchScalarGridSpec(
            num_scalar_prefetch=1,
            grid=(per,),
            in_specs=[
                pl.BlockSpec(gated.shape, lambda j, at: (0, 0)),
                pl.BlockSpec((depth, block), lambda j, at: (0, at[0] * per + j)),
                pl.BlockSpec((depth, block), lambda j, at: (0, total - 1 - at[0] * per - j)),
            ],
            out_specs=pl.BlockSpec((rows, block), lambda j, at: (0, j)),
        ),
        out_shape=jax.ShapeDtypeStruct((rows, wide), F32),
        compiler_params=pltpu.CompilerParams(dimension_semantics=("arbitrary",)),
    )(share.reshape(1).astype(jnp.int32), gated, weight, weight)


def widen(logs):
    return jnp.repeat(jnp.exp(logs), HEADDIM, axis=-1)[..., None, :]


def entering(state, logs, axis):
    n = lax.axis_size(axis)
    me = lax.axis_index(axis)
    top = min(n, 4)
    strides = []
    d = 1
    while n // d > top:
        strides.append(d)
        d *= 2

    def span(first, length):
        return jnp.sum(lax.dynamic_slice_in_dim(logs, first, length, 0), axis=0)

    saved = []
    for d in strides:
        half = state.shape[1] // 2
        upper = (me // d) % 2
        low, high = state[:, :half], state[:, half:]
        mine = jnp.where(upper == 0, low, high)
        other = jnp.where(upper == 0, high, low)
        got = lax.ppermute(other, axis, [(i, i ^ d) for i in range(n)])
        x = jnp.where(upper == 0, mine, got)
        y = jnp.where(upper == 0, got, mine)
        base = (me // (2 * d)) * (2 * d)
        ax = widen(span(base, d))
        ay = widen(span(base + d, d))
        saved.append((d, upper, x, y, ax, ay))
        state = jnp.stack([ay[0] * x[0] + y[0], ax[1] * y[1] + x[1]])
    unit = n // top
    group = me // unit
    padded = jnp.concatenate([jnp.zeros((unit,) + logs.shape[1:], F32), logs,
                              jnp.zeros((unit,) + logs.shape[1:], F32)], axis=0)

    def padded_span(g):
        return jnp.sum(lax.dynamic_slice_in_dim(padded, (g + 1) * unit, unit, 0), axis=0)

    def shift(value, by):
        pairs = [(i, i + by * unit) for i in range(n) if 0 <= i + by * unit < n]
        return lax.ppermute(value, axis, pairs)

    own = padded_span(group)
    before = jnp.stack([padded_span(group - 1)[0], padded_span(group + 1)[1]])
    own_w = widen(own)
    entry = [shift(state[0], 1), shift(state[1], -1)]
    if top > 2:
        summed = [own_w[k] * entry[k] + state[k] for k in (0, 1)]
        fade = widen(before)
        far = [shift(summed[0], 2), shift(summed[1], -2)]
        entry = [fade[k] * far[k] + entry[k] for k in (0, 1)]
    enter = jnp.stack(entry)
    for d, upper, x, y, ax, ay in reversed(saved):
        low = jnp.stack([enter[0], ay[1] * enter[1] + y[1]])
        high = jnp.stack([ax[0] * enter[0] + x[0], enter[1]])
        mine = jnp.where(upper == 0, low, high)
        other = jnp.where(upper == 0, high, low)
        got = lax.ppermute(other, axis, [(i, i ^ d) for i in range(n)])
        enter = jnp.where(
            upper == 0,
            jnp.concatenate([mine, got], axis=1),
            jnp.concatenate([got, mine], axis=1),
        )
    return enter


def by_group(array, heads):
    two, rows, total = array.shape
    cols = array.reshape(two, rows, total // heads, heads)
    return (
        cols.transpose(0, 2, 1, 3).reshape(-1, rows, heads),
        cols.transpose(0, 2, 3, 1).reshape(-1, heads, rows),
    )


def on_device(
    sequence,
    input_weight,
    gate_weight,
    state_weight,
    step_weight,
    step_bias,
    decay_rate,
    skip_gain,
    output_weight,
):
    rows = sequence.shape[0]
    width = input_weight.shape[1]
    head_count = decay_rate.shape[0]
    group = 2 * min(4, width // 128)
    both = stacked(sequence)
    raw = jnp.dot(both, step_weight, preferred_element_type=F32) + step_bias[None, :]
    steps = jax.nn.softplus(raw).astype(BF16).astype(F32).reshape(2, rows, head_count)
    state_proj = jnp.dot(both, state_weight, preferred_element_type=F32).astype(BF16)
    r = lax.broadcasted_iota(jnp.int32, (rows, rows), 0)
    c = lax.broadcasted_iota(jnp.int32, (rows, rows), 1)
    tri = jnp.stack([(r >= c), (r <= c)]).astype(F32)
    ld = jnp.einsum(
        "bts,bsh->bth", tri, -decay_rate[None, None, :] * steps, precision=lax.Precision.HIGHEST
    )
    ends = jnp.stack([ld[0, -1], ld[1, 0]])
    logs = lax.all_gather(ends, "seq")
    factor = jnp.exp(ends[:, None, :] - ld) * steps
    ld_g, ldt_g = by_group(ld, group)
    dt_g, dtt_g = by_group(steps, group)
    factor_g, _ = by_group(factor, group)

    inputs = jnp.dot(both, input_weight, preferred_element_type=F32).astype(BF16)
    state = local_states(inputs, state_proj, factor_g, rows)
    carry = entering(state, logs, "seq")
    gates = jnp.dot(both, gate_weight, preferred_element_type=F32).astype(BF16)
    skip = jnp.repeat(skip_gain, HEADDIM)[None, :]
    inside = inside_of(inputs, state_proj, ld_g, ldt_g, dt_g, dtt_g, skip, rows)
    gated = gated_of(inside, gates, state_proj, ld_g, carry, rows)

    n = lax.axis_size("head")
    me = lax.axis_index("head")
    arrived = []
    for s in range(1, n):
        part = out_share(gated, output_weight, lax.rem(me + s, n), n, rows)
        arrived.append(lax.ppermute(part, "head", [(i, (i + s) % n) for i in range(n)]))
    total = out_share(gated, output_weight, me, n, rows)
    for part in arrived:
        total = total + part
    return total.astype(BF16)


def solution(mesh):
    placed = (
        P("seq", None),
        P(None, "head"),
        P(None, "head"),
        P(),
        P(None, "head"),
        P("head"),
        P("head"),
        P("head"),
        P("head", None),
    )
    return jax.shard_map(
        on_device, mesh=mesh, in_specs=placed, out_specs=P("seq", "head"), check_vma=False
    )
```

```python
import functools

import jax
import jax.numpy as jnp
from jax import lax
from jax.experimental import pallas as pl
from jax.experimental.pallas import tpu as pltpu
from jax.sharding import PartitionSpec as P

F32 = jnp.float32
BF16 = jnp.bfloat16
HEADDIM = 64
CHUNK = 128


def eye_flip(size):
    r = lax.broadcasted_iota(jnp.int32, (size, size), 0)
    c = lax.broadcasted_iota(jnp.int32, (size, size), 1)
    return jnp.where(r + c == size - 1, 1.0, 0.0).astype(BF16)


def flip_kernel(s_ref, o_ref):
    rows, width = s_ref.shape
    block = min(256, width)
    flip = eye_flip(block)
    count = width // block
    o_ref[:rows, :] = s_ref[...]
    for b in range(count):
        src = s_ref[:, (count - 1 - b) * block : (count - b) * block]
        o_ref[rows:, b * block : (b + 1) * block] = jnp.dot(
            src, flip, preferred_element_type=F32
        ).astype(BF16)


def stacked(sequence):
    rows, width = sequence.shape
    return pl.pallas_call(
        flip_kernel,
        out_shape=jax.ShapeDtypeStruct((2 * rows, width), BF16),
    )(sequence)


def pair_wide(cols, first):
    rows = cols.shape[0]
    lane = lax.broadcasted_iota(jnp.int32, (rows, 2 * HEADDIM), 1)
    return jnp.where(lane < HEADDIM, cols[:, first : first + 1], cols[:, first + 1 : first + 2])


def state_kernel(pairs, x_ref, b_ref, w_ref, o_ref):
    writer = b_ref[...]
    factor = w_ref[0]
    parts = []
    for p in range(pairs):
        x = x_ref[:, p * 128 : (p + 1) * 128].astype(F32)
        parts.append((x * pair_wide(factor, 2 * p)).astype(BF16))
    weighted = jnp.concatenate(parts, axis=1)
    o_ref[0] = lax.dot_general(
        writer, weighted, (((0,), (0,)), ((), ())), preferred_element_type=F32
    )


def local_states(inputs, state_proj, factor, rows):
    width = inputs.shape[1]
    state = state_proj.shape[1] // 2
    pairs = min(4, width // 128)
    groups = width // (128 * pairs)
    return pl.pallas_call(
        functools.partial(state_kernel, pairs),
        grid=(2, groups),
        in_specs=[
            pl.BlockSpec((rows, 128 * pairs), lambda d, g: (d, g)),
            pl.BlockSpec((rows, state), lambda d, g: (d, 0)),
            pl.BlockSpec((1, rows, 2 * pairs), lambda d, g: (d * groups + g, 0, 0)),
        ],
        out_specs=pl.BlockSpec((1, state, 128 * pairs), lambda d, g: (d, 0, g)),
        out_shape=jax.ShapeDtypeStruct((2, state, width), F32),
        compiler_params=pltpu.CompilerParams(dimension_semantics=("arbitrary", "arbitrary")),
    )(inputs, state_proj, factor)


def inside_kernel(pairs, state, x_ref, s_ref, ld_ref, ldt_ref, dt_ref, dtt_ref, skip_ref, o_ref, aff):
    branch = pl.program_id(0)
    rows = x_ref.shape[0]
    count = rows // CHUNK
    r = lax.broadcasted_iota(jnp.int32, (CHUNK, CHUNK), 0)
    c = lax.broadcasted_iota(jnp.int32, (CHUNK, CHUNK), 1)

    @pl.when(pl.program_id(1) == 0)
    def _():
        for k in range(count):
            at = slice(k * CHUNK, (k + 1) * CHUNK)
            aff[k] = lax.dot_general(
                s_ref[at, state:], s_ref[at, :state], (((1,), (1,)), ((), ())),
                preferred_element_type=F32,
            )

    lane = lax.broadcasted_iota(jnp.int32, (CHUNK, 128), 1)

    def run(ahead):
        keep = (r >= c) if ahead else (r <= c)
        ld = ld_ref[0]
        ldt = ldt_ref[0]
        dt = dt_ref[0]
        dtt = dtt_ref[0]
        order = range(count) if ahead else range(count - 1, -1, -1)
        carry = jnp.zeros((state, 128 * pairs), F32)
        edge_prev = None
        for step, k in enumerate(order):
            at = slice(k * CHUNK, (k + 1) * CHUNK)
            edge_row = (k + 1) * CHUNK - 1 if ahead else k * CHUNK
            ldk = ld[at, :]
            edge = ld[edge_row : edge_row + 1, :]
            since = jnp.exp(ldk) if step == 0 else jnp.exp(ldk - edge_prev)
            to_end = jnp.exp(edge - ldk) * dt[at, :]
            if step:
                carried = jnp.dot(s_ref[at, state:], carry.astype(BF16), preferred_element_type=F32)
            weighted = []
            for p in range(pairs):
                cols = slice(p * 128, (p + 1) * 128)
                x = x_ref[at, cols]
                xf = x.astype(F32)
                mixes = []
                for h in (2 * p, 2 * p + 1):
                    spread = jnp.where(keep, ldk[:, h : h + 1] - ldt[h : h + 1, at], 0.0)
                    mix = jnp.where(keep, aff[k] * jnp.exp(spread), 0.0) * dtt[h : h + 1, at]
                    mixes.append(mix.astype(BF16))
                zero = jnp.zeros_like(x)
                both = jnp.concatenate(
                    [jnp.where(lane < HEADDIM, x, zero), jnp.where(lane < HEADDIM, zero, x)], axis=0
                )
                out = jnp.dot(jnp.concatenate(mixes, axis=1), both, preferred_element_type=F32)
                out = out + xf * skip_ref[:, cols]
                if step:
                    out = out + carried[:, cols] * pair_wide(since, 2 * p)
                o_ref[at, cols] = out.astype(BF16)
                if step < count - 1:
                    weighted.append((xf * pair_wide(to_end, 2 * p)).astype(BF16))
            if step < count - 1:
                local = lax.dot_general(
                    s_ref[at, :state], jnp.concatenate(weighted, axis=1),
                    (((0,), (0,)), ((), ())), preferred_element_type=F32,
                )
                if step:
                    fade = jnp.exp(edge - edge_prev)
                    wide = jnp.concatenate([pair_wide(fade, 2 * p) for p in range(pairs)], axis=1)
                    carry = carry * wide + local
                else:
                    carry = local
            edge_prev = edge

    @pl.when(branch == 0)
    def _():
        run(True)

    @pl.when(branch == 1)
    def _():
        run(False)


def inside_of(inputs, state_proj, ld, ldt, dt, dtt, skip, rows):
    width = inputs.shape[1]
    state = state_proj.shape[1] // 2
    pairs = min(4, width // 128)
    groups = width // (128 * pairs)
    heads = 2 * pairs
    return pl.pallas_call(
        functools.partial(inside_kernel, pairs, state),
        grid=(2, groups),
        in_specs=[
            pl.BlockSpec((rows, 128 * pairs), lambda d, g: (d, g)),
            pl.BlockSpec((rows, 2 * state), lambda d, g: (d, 0)),
            pl.BlockSpec((1, rows, heads), lambda d, g: (d * groups + g, 0, 0)),
            pl.BlockSpec((1, heads, rows), lambda d, g: (d * groups + g, 0, 0)),
            pl.BlockSpec((1, rows, heads), lambda d, g: (d * groups + g, 0, 0)),
            pl.BlockSpec((1, heads, rows), lambda d, g: (d * groups + g, 0, 0)),
            pl.BlockSpec((1, 128 * pairs), lambda d, g: (0, g)),
        ],
        out_specs=pl.BlockSpec((rows, 128 * pairs), lambda d, g: (d, g)),
        out_shape=jax.ShapeDtypeStruct(inputs.shape, BF16),
        scratch_shapes=[pltpu.VMEM((rows // CHUNK, CHUNK, CHUNK), F32)],
        compiler_params=pltpu.CompilerParams(dimension_semantics=("arbitrary", "arbitrary")),
    )(inputs, state_proj, ld, ldt, dt, dtt, skip)


def gate_kernel(pairs, state, i_ref, g_ref, s_ref, ld_ref, c_ref, o_ref):
    reader = s_ref[:, state:]
    carried = jnp.dot(reader, c_ref[0].astype(BF16), preferred_element_type=F32)
    grown = jnp.exp(ld_ref[0])
    for p in range(pairs):
        cols = slice(p * 128, (p + 1) * 128)
        g = g_ref[:, cols].astype(F32)
        full = i_ref[:, cols].astype(F32) + carried[:, cols] * pair_wide(grown, 2 * p)
        o_ref[:, cols] = (full * (g / (1.0 + jnp.exp(-g)))).astype(BF16)


def gated_of(inside, gates, state_proj, ld, carry, rows):
    width = inside.shape[1]
    state = state_proj.shape[1] // 2
    pairs = min(4, width // 128)
    groups = width // (128 * pairs)
    heads = 2 * pairs
    tile = pl.BlockSpec((rows, 128 * pairs), lambda d, g: (d, g))
    return pl.pallas_call(
        functools.partial(gate_kernel, pairs, state),
        grid=(2, groups),
        in_specs=[
            tile,
            tile,
            pl.BlockSpec((rows, 2 * state), lambda d, g: (d, 0)),
            pl.BlockSpec((1, rows, heads), lambda d, g: (d * groups + g, 0, 0)),
            pl.BlockSpec((1, state, 128 * pairs), lambda d, g: (d, 0, g)),
        ],
        out_specs=tile,
        out_shape=jax.ShapeDtypeStruct(inside.shape, BF16),
        compiler_params=pltpu.CompilerParams(dimension_semantics=("arbitrary", "arbitrary")),
    )(inside, gates, state_proj, ld, carry)


def out_kernel(rows, at_ref, g_ref, w_ref, v_ref, o_ref):
    flipped = jnp.dot(v_ref[...], eye_flip(v_ref.shape[1]), preferred_element_type=F32).astype(BF16)
    acc = jnp.dot(g_ref[:rows, :], w_ref[...], preferred_element_type=F32)
    o_ref[...] = acc + jnp.dot(g_ref[rows:, :], flipped, preferred_element_type=F32)


def out_share(gated, weight, share, shares, rows):
    depth, columns = weight.shape
    wide = columns // shares
    block = min(256, wide)
    per = wide // block
    total = columns // block
    return pl.pallas_call(
        functools.partial(out_kernel, rows),
        grid_spec=pltpu.PrefetchScalarGridSpec(
            num_scalar_prefetch=1,
            grid=(per,),
            in_specs=[
                pl.BlockSpec(gated.shape, lambda j, at: (0, 0)),
                pl.BlockSpec((depth, block), lambda j, at: (0, at[0] * per + j)),
                pl.BlockSpec((depth, block), lambda j, at: (0, total - 1 - at[0] * per - j)),
            ],
            out_specs=pl.BlockSpec((rows, block), lambda j, at: (0, j)),
        ),
        out_shape=jax.ShapeDtypeStruct((rows, wide), F32),
        compiler_params=pltpu.CompilerParams(dimension_semantics=("arbitrary",)),
    )(share.reshape(1).astype(jnp.int32), gated, weight, weight)


def widen(logs):
    return jnp.repeat(jnp.exp(logs), HEADDIM, axis=-1)[..., None, :]


def entering(state, own, gate_of, inside_from, axis):
    n = lax.axis_size(axis)
    me = lax.axis_index(axis)
    top = min(n, 4)
    strides = []
    d = 1
    while n // d > top:
        strides.append(d)
        d *= 2

    saved = []
    tied = None if strides else gate_of(state)[1]
    for d in strides:
        if d == strides[-1]:
            state, tied = gate_of(state)
        half = state.shape[1] // 2
        upper = (me // d) % 2
        low, high = state[:, :half], state[:, half:]
        mine = jnp.where(upper == 0, low, high)
        other = jnp.where(upper == 0, high, low)
        got = lax.ppermute(other, axis, [(i, i ^ d) for i in range(n)])
        x = jnp.where(upper == 0, mine, got)
        y = jnp.where(upper == 0, got, mine)
        got_log = lax.ppermute(own, axis, [(i, i ^ d) for i in range(n)])
        ax = widen(jnp.where(upper == 0, own, got_log))
        ay = widen(jnp.where(upper == 0, got_log, own))
        own = own + got_log
        saved.append((d, upper, x, y, ax, ay))
        state = jnp.stack([ay[0] * x[0] + y[0], ax[1] * y[1] + x[1]])
    unit = n // top
    gates = tied
    state, gates = lax.optimization_barrier((state, gates))

    def shift(value, by):
        pairs = [(i, i + by * unit) for i in range(n) if 0 <= i + by * unit < n]
        return lax.ppermute(value, axis, pairs)

    before = jnp.stack([shift(own[0], 1), shift(own[1], -1)])
    own_w = widen(own)
    entry = [shift(state[0], 1), shift(state[1], -1)]
    if top > 2:
        summed = [own_w[k] * entry[k] + state[k] for k in (0, 1)]
        fade = widen(before)
        far = [shift(summed[0], 2), shift(summed[1], -2)]
        entry = [fade[k] * far[k] + entry[k] for k in (0, 1)]
    enter = jnp.stack(entry)
    enter, inside = inside_from(enter)
    first = True
    for d, upper, x, y, ax, ay in reversed(saved):
        low = jnp.stack([enter[0], ay[1] * enter[1] + y[1]])
        high = jnp.stack([ax[0] * enter[0] + x[0], enter[1]])
        mine = jnp.where(upper == 0, low, high)
        other = jnp.where(upper == 0, high, low)
        if not first:
            other, inside = lax.optimization_barrier((other, inside))
        first = False
        got = lax.ppermute(other, axis, [(i, i ^ d) for i in range(n)])
        enter = jnp.where(
            upper == 0,
            jnp.concatenate([mine, got], axis=1),
            jnp.concatenate([got, mine], axis=1),
        )
    return enter, gates, inside


def by_group(array, heads):
    two, rows, total = array.shape
    cols = array.reshape(two, rows, total // heads, heads)
    return (
        cols.transpose(0, 2, 1, 3).reshape(-1, rows, heads),
        cols.transpose(0, 2, 3, 1).reshape(-1, heads, rows),
    )


def on_device(
    sequence,
    input_weight,
    gate_weight,
    state_weight,
    step_weight,
    step_bias,
    decay_rate,
    skip_gain,
    output_weight,
):
    rows = sequence.shape[0]
    width = input_weight.shape[1]
    head_count = decay_rate.shape[0]
    group = 2 * min(4, width // 128)
    both = stacked(sequence)
    raw = jnp.dot(both, step_weight, preferred_element_type=F32) + step_bias[None, :]
    steps = jax.nn.softplus(raw).astype(BF16).astype(F32).reshape(2, rows, head_count)
    state_proj = jnp.dot(both, state_weight, preferred_element_type=F32).astype(BF16)
    r = lax.broadcasted_iota(jnp.int32, (rows, rows), 0)
    c = lax.broadcasted_iota(jnp.int32, (rows, rows), 1)
    tri = jnp.stack([(r >= c), (r <= c)]).astype(F32)
    ld = jnp.einsum(
        "bts,bsh->bth", tri, -decay_rate[None, None, :] * steps, precision=lax.Precision.HIGHEST
    )
    ends = jnp.stack([ld[0, -1], ld[1, 0]])
    factor = jnp.exp(ends[:, None, :] - ld) * steps
    ld_g, ldt_g = by_group(ld, group)
    dt_g, dtt_g = by_group(steps, group)
    factor_g, _ = by_group(factor, group)

    inputs = jnp.dot(both, input_weight, preferred_element_type=F32).astype(BF16)
    state = local_states(inputs, state_proj, factor_g, rows)
    skip = jnp.repeat(skip_gain, HEADDIM)[None, :]

    def gate_of(after):
        after, source = lax.optimization_barrier((after, both))
        return after, jnp.dot(source, gate_weight, preferred_element_type=F32).astype(BF16)

    def inside_from(after):
        after, source = lax.optimization_barrier((after, inputs))
        return after, inside_of(source, state_proj, ld_g, ldt_g, dt_g, dtt_g, skip, rows)

    carry, gates, inside = entering(state, ends, gate_of, inside_from, "seq")
    gated = gated_of(inside, gates, state_proj, ld_g, carry, rows)

    n = lax.axis_size("head")
    me = lax.axis_index("head")
    arrived = []
    cuts = 2
    for s in range(1, n):
        peer = lax.rem(me + s, n)
        pieces = []
        for k in range(cuts):
            part = out_share(gated, output_weight, cuts * peer + k, cuts * n, rows)
            pieces.append(lax.ppermute(part, "head", [(i, (i + s) % n) for i in range(n)]))
        arrived.append(jnp.concatenate(pieces, axis=1))
    total = out_share(gated, output_weight, me, n, rows)
    for part in arrived:
        total = total + part
    return total.astype(BF16)


def solution(mesh):
    placed = (
        P("seq", None),
        P(None, "head"),
        P(None, "head"),
        P(),
        P(None, "head"),
        P("head"),
        P("head"),
        P("head"),
        P("head", None),
    )
    return jax.shard_map(
        on_device, mesh=mesh, in_specs=placed, out_specs=P("seq", "head"), check_vma=False
    )
```
